32 devices in a mesh: row: 8 (over z, core), col: 4 (over y, x).
Axes of the slice: x: 2, y: 2, z: 4, core: 2. Of those that a mesh axis runs over, the one named last changes fastest.
Arguments:
- flow_tiles: bfloat16 [8, 8, 256, 256], P('row', 'col'), may hold values from 0.1 to 25
- tile_cols: int32 [8, 8], P('row', 'col'), may hold values from -1 to 7, as said below
- pairs: int32 [512, 2], P(('row', 'col')), may hold values from -1 to 7, as said below
Outputs:
- new_flow: float32 [8, 8, 256, 256], P('row', 'col')
The draws below stay inside these ranges and needn't reach their ends.
Inputs may be any that keep to these rules, and one draw needn't show every extreme that they name: `tile_cols`: the stored slots of device (r, c) have distinct tile columns, each congruent to c modulo the col axis's size; tile row r stores tile column r. `pairs`: device (r, c) lists, in some order and without repeats, exactly the (k, s) for which slot s of the device is stored and M[r, k] and M[k, tile_cols[r, c * 2 + s]] are both stored tiles; its other rows are (-1, -1). Some device uses all 16 rows.
All inputs are finite; a program needn't handle non-finite values.
Results may differ from the reference program's by a relative error of at most 0.0003.
Values may be sent and summed in bfloat16 or wider, within the bound.
A program may use at most 64 MiB of HBM per device.

```python
import jax
import jax.numpy as jnp
from jax import lax

B = 256
NB = 8
TPD = 2
PPD = 16
N_COL = 4


def draw_flow_tiles(key, part):
    second_key = jax.random.fold_in(key, 1)
    row_values = jnp.arange(NB, dtype=jnp.float32)
    row_scale = 3.0 ** (row_values / jnp.float32(max(NB - 1, 1)))
    normal_part = jnp.clip(jax.random.normal(second_key, (NB, NB, B, B), jnp.float32), -4.0, 4.0)
    magnitude = jnp.exp(0.5 * normal_part)
    return (magnitude * row_scale[:, None, None, None]).astype(jnp.bfloat16)


def block_pattern(key):
    perm_key, keep_key, row_key, col_key = jax.random.split(jax.random.fold_in(key, 11), 4)
    subkeys = jax.random.split(perm_key, NB * N_COL)
    orders = jax.vmap(lambda subkey: jax.random.permutation(subkey, TPD))(subkeys)
    columns = jnp.arange(N_COL, dtype=jnp.int32)[None, :, None] + N_COL * orders.reshape(NB, N_COL, TPD).astype(jnp.int32)
    columns = columns.reshape(NB, NB).astype(jnp.int32)
    keep = jax.random.randint(keep_key, (NB, NB), 0, 2).astype(jnp.int32) > 0
    special_row = jax.random.randint(row_key, (), 0, NB).astype(jnp.int32)
    special_col = jax.random.randint(col_key, (), 0, N_COL).astype(jnp.int32)
    special_cols = jax.lax.dynamic_slice_in_dim(columns[special_row], special_col * TPD, TPD, 0)
    indices = jnp.arange(NB, dtype=jnp.int32)
    is_special_col = jnp.any(special_cols[None, :] == indices[:, None], axis=1)
    stored = keep | (indices[:, None] == indices[None, :]) | (indices[:, None] == special_row) | is_special_col[None, :]
    slot_stored = jnp.take_along_axis(stored, columns, axis=1)
    tile_cols = jnp.where(slot_stored, columns, -1).astype(jnp.int32)
    return (columns, stored, tile_cols)


def draw_tile_cols(key, part):
    columns, stored, tile_cols = block_pattern(key)
    return tile_cols


def draw_pairs(key, part):
    columns, stored, tile_cols = block_pattern(key)
    device_cols = columns.reshape(NB, N_COL, TPD)
    slot_stored = tile_cols.reshape(NB, N_COL, TPD) >= 0
    left_ok = stored[:, None, None, :]
    right_ok = stored.T[device_cols]
    valid = slot_stored[:, :, :, None] & left_ok & right_ok
    valid = valid.reshape(NB, N_COL, PPD)
    index_list = jnp.arange(PPD, dtype=jnp.int32)
    score = jnp.where(valid, index_list, index_list + PPD).astype(jnp.int32)
    order = jnp.argsort(score, axis=-1).astype(jnp.int32)
    valid_sorted = jnp.take_along_axis(valid, order, axis=-1)
    inner_tile = jnp.where(valid_sorted, order % NB, -1)
    slot_table = jnp.where(valid_sorted, order // NB, -1)
    return jnp.stack([inner_tile, slot_table], axis=-1).reshape(NB * N_COL * PPD, 2).astype(jnp.int32)


def setup_inputs(seed: int = 0) -> dict:
    keys = jax.random.split(jax.random.key(seed), 4)
    return {
        "flow_tiles": draw_flow_tiles(jax.random.fold_in(keys[3], 71), 0),
        "tile_cols": draw_tile_cols(jax.random.fold_in(keys[3], 71), 0),
        "pairs": draw_pairs(jax.random.fold_in(keys[3], 71), 0),
    }


def reference(flow_tiles, tile_cols, pairs):
    column_ids = jnp.arange(NB, dtype=jnp.int32)
    matching = tile_cols[:, None, :] == column_ids[None, :, None]
    present = jnp.any(matching, axis=2)
    position = jnp.argmax(matching, axis=2).astype(jnp.int32)
    taken = jnp.take_along_axis(flow_tiles, position[:, :, None, None], axis=1)
    ordered = jnp.where(present[:, :, None, None], taken, jnp.zeros((), flow_tiles.dtype))
    pair_table = pairs.reshape(NB, N_COL, PPD, 2)
    slot_ids = jnp.arange(TPD, dtype=jnp.int32)

    def one_row(row_id):
        def one_device(col_id):
            inner_tile = pair_table[row_id, col_id, :, 0]
            slot_list = pair_table[row_id, col_id, :, 1]
            is_live = inner_tile >= 0
            inner_safe = jnp.maximum(inner_tile, 0)
            slot_safe = jnp.maximum(slot_list, 0)
            wanted = jnp.maximum(tile_cols[row_id, col_id * TPD + slot_safe], 0)
            left_tiles = ordered[row_id, inner_safe].astype(jnp.float32)
            right_tiles = ordered[inner_safe, wanted].astype(jnp.float32)
            products = jnp.einsum('pab,pbc->pac', left_tiles, right_tiles, precision=lax.Precision.HIGHEST)
            weight = (is_live[:, None] & (slot_list[:, None] == slot_ids[None, :])).astype(jnp.float32)
            return jnp.einsum('ps,pac->sac', weight, products, precision=lax.Precision.HIGHEST)
        return lax.map(one_device, jnp.arange(N_COL, dtype=jnp.int32))

    expanded = lax.map(one_row, jnp.arange(NB, dtype=jnp.int32)).reshape(NB, NB, B, B)
    inflated = expanded * expanded
    inflated_ordered = jnp.take_along_axis(inflated, position[:, :, None, None], axis=1)
    inflated_ordered = jnp.where(present[:, :, None, None], inflated_ordered, 0.0)
    totals = jnp.sum(inflated_ordered, axis=(0, 2))
    stored = tile_cols >= 0
    divisor = totals[jnp.maximum(tile_cols, 0)]
    divisor = jnp.where(stored[:, :, None], divisor, 1.0)
    normed = inflated * jnp.float32(NB * B) / divisor[:, :, None, :]
    blended = 0.5 * flow_tiles.astype(jnp.float32) + 0.5 * normed
    return jnp.where(stored[:, :, None, None], blended, 0.0)
```

```python
import functools
import math

import jax
import jax.numpy as jnp
from jax import lax
from jax.experimental import pallas as pl
from jax.experimental.pallas import tpu as pltpu
from jax.sharding import PartitionSpec as P

MESH = pl.DeviceIdType.MESH
CORES = 2
SPLIT = 2


def remote(src, dst, send_sem, recv_sem, device):
    return pltpu.make_async_remote_copy(
        src_ref=src,
        dst_ref=dst,
        send_sem=send_sem,
        recv_sem=recv_sem,
        device_id=device,
        device_id_type=MESH,
    )


def kernel(
    nrow, ncol, cols_ref, flow_ref, out_ref,
    own, blocks, left, acc, sums,
    up_send, dn_send, mate_send, recv, col_send, col_recv, sum_send, sum_recv,
):
    tiles, width = flow_ref.shape[1], flow_ref.shape[3]
    chunks, depth = own.shape[0], own.shape[1]
    planes = nrow // CORES
    row, col = lax.axis_index("row"), lax.axis_index("col")
    z, core = row // CORES, row % CORES
    mate = (row + 1 - 2 * core, col)
    above, below = (row + CORES, col), (row - CORES, col)
    has_above, has_below = z < planes - 1, z > 0
    ny = math.isqrt(ncol)
    ny = ny if ny * ny == ncol else 1
    nx = ncol // ny
    y, x = col // nx, col % nx
    peers = []
    for dy in range(ny):
        for dx in range(nx):
            if dy or dx:
                peers.append((dy * nx + dx, ((y + dy) % ny) * nx + (x + dx) % nx))
    peers.sort(key=lambda p: (p[0] // nx > 0) + (p[0] % nx > 0))

    barrier = pltpu.get_barrier_semaphore()

    def greet(device):
        pl.semaphore_signal(barrier, inc=1, device_id=device, device_id_type=MESH)

    greet(mate)
    for _, peer in peers:
        greet((row, peer))

    @pl.when(has_above)
    def _():
        greet(above)

    @pl.when(has_below)
    def _():
        greet(below)

    kept = []
    for t in range(tiles):
        target = col + ncol * t
        tile = jnp.zeros((width, width), jnp.float32)
        weight = jnp.float32(0)
        for s in range(tiles):
            w = (cols_ref[0, s] == target).astype(jnp.float32)
            weight = weight + w
            tile = tile + flow_ref[0, s].astype(jnp.float32) * w
        kept.append(weight)
        tile = tile.astype(jnp.bfloat16)
        own[t * SPLIT:(t + 1) * SPLIT] = tile.reshape(SPLIT, depth, width)
        left[col, t] = tile
    blocks[row] = own[...]

    ends = jnp.where(has_above, 1, 0) + jnp.where(has_below, 1, 0)
    pl.semaphore_wait(barrier, ncol + ends)

    def to_above(step, k, q, src):
        return remote(src, blocks.at[k, q], up_send.at[step, q], recv.at[k, q], above)

    def to_below(step, k, q, src):
        return remote(src, blocks.at[k, q], dn_send.at[step, q], recv.at[k, q], below)

    def to_mate(plane, k, q, src):
        return remote(src, blocks.at[k, q], mate_send.at[plane, q], recv.at[k, q], mate)

    def arrived(k, q):
        remote(own.at[q], blocks.at[k, q], mate_send.at[0, q], recv.at[k, q], mate).wait_recv()

    def to_peer(slot, peer):
        return remote(
            blocks_as_tiles(), left.at[col], col_send.at[slot], col_recv.at[col], (row, peer)
        )

    def blocks_as_tiles():
        return left.at[col]

    for q in range(chunks):

        @pl.when(has_above)
        def _():
            to_above(0, row, q, own.at[q]).start()

        @pl.when(has_below)
        def _():
            to_below(0, row, q, own.at[q]).start()

        if q == 0:
            for slot, peer in peers:
                to_peer(slot, peer).start()
        to_mate(z, row, q, own.at[q]).start()

    acc[...] = jnp.zeros_like(acc)

    def relay(step, q):
        @pl.when(z >= step)
        def _():
            k = row - CORES * step
            arrived(k, q)

            @pl.when(has_above)
            def _():
                to_above(step, k, q, blocks.at[k, q]).start()

            to_mate(z - step, k, q, blocks.at[k, q]).start()

        @pl.when(z + step < planes)
        def _():
            k = row + CORES * step
            arrived(k, q)

            @pl.when(has_below)
            def _():
                to_below(step, k, q, blocks.at[k, q]).start()

            to_mate(z + step, k, q, blocks.at[k, q]).start()

    def multiply(k):
        a = left[k % ncol, k // ncol]
        for t in range(tiles):
            b = blocks[k, pl.ds(t * SPLIT, SPLIT)].reshape(width, width)
            acc[t] += jnp.dot(a, b, preferred_element_type=jnp.float32)

    def multiply_chunk(k, q):
        part = pl.ds((q % SPLIT) * depth, depth)
        a = left[k % ncol, k // ncol, :, part]
        acc[q // SPLIT] += jnp.dot(a, blocks[k, q], preferred_element_type=jnp.float32)

    def compute(distance):
        for sign in (-1, 1) if distance else (1,):
            plane = z + sign * distance

            @pl.when((plane >= 0) & (plane < planes))
            def _():
                mine = plane * CORES + core
                multiply(mine)
                other = plane * CORES + 1 - core
                for q in range(chunks):
                    arrived(other, q)
                multiply(other)

    def last(distance):
        for sign in (-1, 1):
            plane = z + sign * distance

            @pl.when((plane >= 0) & (plane < planes))
            def _():
                mine = plane * CORES + core
                other = plane * CORES + 1 - core
                for q in range(chunks):
                    arrived(mine, q)
                    to_mate(plane, mine, q, blocks.at[mine, q]).start()
                    multiply_chunk(mine, q)
                    if q:
                        arrived(other, q - 1)
                        multiply_chunk(other, q - 1)
                arrived(other, chunks - 1)
                multiply_chunk(other, chunks - 1)

    done = 0

    def catch_up(upto):
        nonlocal done
        if done == 0:
            for slot, peer in peers:
                remote(
                    left.at[peer], left.at[peer], col_send.at[slot], col_recv.at[peer], (row, peer)
                ).wait_recv()
        while done < upto:
            compute(done)
            done += 1

    for step in range(1, planes - 1):
        if step > 2:
            catch_up(step)
        for q in range(chunks):
            relay(step, q)
    catch_up(planes - 1)
    last(planes - 1)

    for t in range(tiles):
        squares = acc[t] * acc[t]
        acc[t] = squares
        sums[row, t] = jnp.sum(squares, axis=0) * kept[t]

    def to_row(d):
        other = (row + d) % nrow
        return other, remote(
            sums.at[row], sums.at[row], sum_send.at[d], sum_recv.at[row], (other, col)
        )

    for d in range(1, nrow):
        to_row(d)[1].start()
    for d in range(1, nrow):
        other, _ = to_row(d)
        remote(
            sums.at[other], sums.at[other], sum_send.at[d], sum_recv.at[other], (other, col)
        ).wait_recv()
    totals = sums[0]
    for k in range(1, nrow):
        totals = totals + sums[k]
    for s in range(tiles):
        out = jnp.zeros((width, width), jnp.float32)
        held = jnp.float32(0)
        for t in range(tiles):
            w = (cols_ref[0, s] == col + ncol * t).astype(jnp.float32)
            held = held + w
            safe = jnp.where(totals[t] > 0, totals[t], 1.0)
            scale = jnp.float32(0.5 * nrow * width) / safe * w
            out = out + acc[t] * scale[None, :]
        out_ref[0, s] = out + flow_ref[0, s].astype(jnp.float32) * (0.5 * held)

    for q in range(chunks):
        for step in range(planes):
            @pl.when(has_above & (z >= step))
            def _():
                to_above(step, row, q, own.at[q]).wait_send()

            @pl.when(has_below & (z + step < planes))
            def _():
                to_below(step, row, q, own.at[q]).wait_send()

            to_mate(step, row, q, own.at[q]).wait_send()
    for slot, peer in peers:
        to_peer(slot, peer).wait_send()
    for d in range(1, nrow):
        to_row(d)[1].wait_send()


def on_device(nrow, ncol, flow_tiles, tile_cols, pairs):
    _, tiles, _, width = flow_tiles.shape
    planes, chunks, depth = nrow // CORES, tiles * SPLIT, width // SPLIT
    dma = pltpu.SemaphoreType.DMA
    return pl.pallas_call(
        functools.partial(kernel, nrow, ncol),
        out_shape=jax.ShapeDtypeStruct(flow_tiles.shape, jnp.float32),
        in_specs=[
            pl.BlockSpec(memory_space=pltpu.SMEM),
            pl.BlockSpec(memory_space=pltpu.VMEM),
        ],
        out_specs=pl.BlockSpec(memory_space=pltpu.VMEM),
        scratch_shapes=[
            pltpu.VMEM((chunks, depth, width), jnp.bfloat16),
            pltpu.VMEM((nrow, chunks, depth, width), jnp.bfloat16),
            pltpu.VMEM((ncol, tiles, width, width), jnp.bfloat16),
            pltpu.VMEM((tiles, width, width), jnp.float32),
            pltpu.VMEM((nrow, tiles, width), jnp.float32),
            dma((planes, chunks)),
            dma((planes, chunks)),
            dma((planes, chunks)),
            dma((nrow, chunks)),
            dma((ncol,)),
            dma((ncol,)),
            dma((nrow,)),
            dma((nrow,)),
        ],
        compiler_params=pltpu.CompilerParams(
            collective_id=0, has_side_effects=True, vmem_limit_bytes=48 * 1024 * 1024
        ),
        name="cluster_step",
    )(tile_cols, flow_tiles)


def solution(mesh):
    placed = (P("row", "col", None, None), P("row", "col"), P(("row", "col"), None))
    return jax.shard_map(
        functools.partial(on_device, mesh.shape["row"], mesh.shape["col"]),
        mesh=mesh,
        in_specs=placed,
        out_specs=P("row", "col", None, None),
        check_vma=False,
    )
```

```python
import functools
import math

import jax
import jax.numpy as jnp
from jax import lax
from jax.experimental import pallas as pl
from jax.experimental.pallas import tpu as pltpu
from jax.sharding import PartitionSpec as P

MESH = pl.DeviceIdType.MESH
CORES = 2
SPLIT = 2


def remote(src, dst, send_sem, recv_sem, device):
    return pltpu.make_async_remote_copy(
        src_ref=src,
        dst_ref=dst,
        send_sem=send_sem,
        recv_sem=recv_sem,
        device_id=device,
        device_id_type=MESH,
    )


def kernel(
    nrow, ncol, cols_hbm, flow_hbm, out_ref,
    cols, raw, own, blocks, left, acc, swap, result, flags, sums,
    in_sem, up_send, dn_send, mate_send, recv, left_send, left_recv,
    left_mate, flag_sem, swap_sem, sum_send, sum_recv,
):
    tiles, width = raw.shape[0], raw.shape[2]
    depth = own.shape[1]
    share = tiles // CORES
    pieces = share * SPLIT
    planes = nrow // CORES
    row, col = lax.axis_index("row"), lax.axis_index("col")
    z, core = row // CORES, row % CORES
    mate = (row + 1 - 2 * core, col)
    mate_row = row + 1 - 2 * core
    above, below = (row + CORES, col), (row - CORES, col)
    has_above, has_below = z < planes - 1, z > 0
    ny = math.isqrt(ncol)
    ny = ny if ny * ny == ncol else 1
    nx = ncol // ny
    y, x = col // nx, col % nx
    peers = []
    for dy in range(ny):
        for dx in range(nx):
            if dy or dx:
                peers.append((dy * nx + dx, ((y + dy) % ny) * nx + (x + dx) % nx))
    peers.sort(key=lambda p: (p[0] // nx > 0) + (p[0] % nx > 0))

    load_cols = pltpu.make_async_copy(cols_hbm, cols, in_sem.at[0])
    load_flow = pltpu.make_async_copy(flow_hbm.at[0], raw, in_sem.at[1])
    load_cols.start()
    load_flow.start()

    barrier = pltpu.get_barrier_semaphore()

    def greet(device):
        pl.semaphore_signal(barrier, inc=1, device_id=device, device_id_type=MESH)

    greet(mate)
    for _, peer in peers:
        greet((row, peer))

    @pl.when(has_above)
    def _():
        for c in range(CORES):
            greet(((z + 1) * CORES + c, col))

    @pl.when(has_below)
    def _():
        for c in range(CORES):
            greet(((z - 1) * CORES + c, col))

    load_cols.wait()
    load_flow.wait()
    for t in range(tiles):
        target = col + ncol * t
        tile = jnp.zeros((width, width), jnp.float32)
        weight = jnp.float32(0)
        for s in range(tiles):
            w = (cols[0, s] == target).astype(jnp.float32)
            weight = weight + w
            tile = tile + raw[s].astype(jnp.float32) * w
        flags[core, t] = jnp.full((width,), weight, jnp.float32)
        tile = tile.astype(jnp.bfloat16)
        own[t * SPLIT:(t + 1) * SPLIT] = tile.reshape(SPLIT, depth, width)
        left[col, t, core] = tile
    blocks[row] = own[pl.ds(core * pieces, pieces)]

    ends = jnp.where(has_above, 1, 0) + jnp.where(has_below, 1, 0)
    pl.semaphore_wait(barrier, ncol + CORES * ends)

    def piece(src, k, u, send_sem, device):
        return remote(src, blocks.at[k, u], send_sem, recv.at[k, u], device)

    def arrived(k, u):
        piece(own.at[u], k, u, mate_send.at[u], mate).wait_recv()

    def to_mate(u):
        return piece(own.at[(1 - core) * pieces + u], row, u, mate_send.at[u], mate)

    def left_copy(slot, c, rc, device, send_sem):
        part = left.at[c, :, rc]
        return remote(part, part, send_sem, left_recv.at[rc, c], device)

    flag_copy = remote(flags.at[core], flags.at[core], flag_sem.at[0], flag_sem.at[1], mate)

    for u in range(pieces):
        for c in range(CORES):

            @pl.when(has_above)
            def _():
                piece(
                    own.at[c * pieces + u], row, u, up_send.at[0, c * pieces + u],
                    ((z + 1) * CORES + c, col),
                ).start()

            @pl.when(has_below)
            def _():
                piece(
                    own.at[c * pieces + u], row, u, dn_send.at[0, c * pieces + u],
                    ((z - 1) * CORES + c, col),
                ).start()

        if u == 0:
            for slot, peer in peers:
                left_copy(slot, col, core, (row, peer), left_send.at[slot]).start()
    for u in range(pieces):
        to_mate(u).start()
    left_copy(0, col, core, mate, left_mate.at[col]).start()
    flag_copy.start()

    acc[...] = jnp.zeros_like(acc)

    def relay(step):
        for c in range(CORES):
            for u in range(pieces):

                @pl.when(z >= step)
                def _():
                    k = (z - step) * CORES + c
                    arrived(k, u)

                    @pl.when(has_above)
                    def _():
                        piece(
                            blocks.at[k, u], k, u, up_send.at[step, c * pieces + u], above
                        ).start()

                @pl.when(z + step < planes)
                def _():
                    k = (z + step) * CORES + c
                    arrived(k, u)

                    @pl.when(has_below)
                    def _():
                        piece(
                            blocks.at[k, u], k, u, dn_send.at[step, c * pieces + u], below
                        ).start()

    def multiply(k):
        a = left[k % ncol, k // ncol].reshape(CORES * width, width)
        for i in range(share):
            b = blocks[k, pl.ds(i * SPLIT, SPLIT)].reshape(width, width)
            c = jnp.dot(a, b, preferred_element_type=jnp.float32)
            acc[i] += c.reshape(CORES, width, width)

    def multiply_piece(k, u):
        h = u % SPLIT
        a = left[k % ncol, k // ncol, :, :, pl.ds(h * depth, depth)]
        c = jnp.dot(
            a.reshape(CORES * width, depth), blocks[k, u], preferred_element_type=jnp.float32
        )
        acc[u // SPLIT] += c.reshape(CORES, width, width)

    def compute(distance):
        for sign in (-1, 1) if distance else (1,):
            plane = z + sign * distance

            @pl.when((plane >= 0) & (plane < planes))
            def _():
                if distance == 0:
                    for u in range(pieces):
                        arrived(mate_row, u)
                for c in range(CORES):
                    multiply(plane * CORES + c)

    def last(distance):
        for sign in (-1, 1):
            plane = z + sign * distance

            @pl.when((plane >= 0) & (plane < planes))
            def _():
                for c in range(CORES):
                    for u in range(pieces):
                        k = plane * CORES + c
                        arrived(k, u)
                        multiply_piece(k, u)

    done = 0

    def catch_up(upto):
        nonlocal done
        if done == 0:
            for slot, peer in peers:
                left_copy(slot, peer, core, mate, left_mate.at[peer]).wait_recv()
                left_copy(slot, peer, core, mate, left_mate.at[peer]).start()
            for c in range(ncol):
                left_copy(0, c, 1 - core, mate, left_mate.at[c]).wait_recv()
        while done < upto:
            compute(done)
            done += 1

    for step in range(1, planes - 1):
        if step > 2:
            catch_up(step)
        relay(step)
    catch_up(planes - 1)
    last(planes - 1)
    flag_copy.wait_recv()

    for i in range(share):
        t = core * share + i
        part = jnp.zeros((width,), jnp.float32)
        for c in range(CORES):
            part = part + jnp.sum(acc[i, c] * acc[i, c], axis=0) * flags[c, t]
        sums[row, i] = part

    def to_row(d):
        return remote(
            sums.at[row], sums.at[row], sum_send.at[d], sum_recv.at[row],
            ((row + d) % nrow, col),
        )

    for d in range(1, nrow):
        to_row(d).start()

    for i in range(share):
        other = acc[i, 1 - core]
        swap[i] = other * other
    swap_copy = remote(
        swap, result.at[pl.ds(core * share, share)], swap_sem.at[0], swap_sem.at[1], mate
    )
    swap_copy.start()
    for i in range(share):
        mine = acc[i, core]
        result[core * share + i] = mine * mine
    swap_copy.wait_recv()

    for d in range(1, nrow):
        other = (row + d) % nrow
        remote(
            sums.at[other], sums.at[other], sum_send.at[d], sum_recv.at[other], (other, col)
        ).wait_recv()
    for s in range(tiles):
        out = jnp.zeros((width, width), jnp.float32)
        held = jnp.float32(0)
        for t in range(tiles):
            w = (cols[0, s] == col + ncol * t).astype(jnp.float32)
            held = held + w
            total = sums[t // share, t % share]
            for p in range(1, planes):
                total = total + sums[p * CORES + t // share, t % share]
            safe = jnp.where(total > 0, total, 1.0)
            scale = jnp.float32(0.5 * nrow * width) / safe * w
            out = out + result[t] * scale[None, :]
        out_ref[0, s] = out + raw[s].astype(jnp.float32) * (0.5 * held)
    for n in range(CORES * pieces):
        for step in range(planes):

            @pl.when(has_above & (z >= step))
            def _():
                piece(own.at[n], row, 0, up_send.at[step, n], above).wait_send()

            @pl.when(has_below & (z + step < planes))
            def _():
                piece(own.at[n], row, 0, dn_send.at[step, n], below).wait_send()

    for u in range(pieces):
        to_mate(u).wait_send()
    for slot, peer in peers:
        left_copy(slot, col, core, (row, peer), left_send.at[slot]).wait_send()
    for c in range(ncol):
        left_copy(0, c, core, mate, left_mate.at[c]).wait_send()
    flag_copy.wait_send()
    swap_copy.wait_send()
    for d in range(1, nrow):
        to_row(d).wait_send()


def on_device(nrow, ncol, flow_tiles, tile_cols, pairs):
    _, tiles, _, width = flow_tiles.shape
    planes, depth, share = nrow // CORES, width // SPLIT, tiles // CORES
    pieces = share * SPLIT
    dma = pltpu.SemaphoreType.DMA
    return pl.pallas_call(
        functools.partial(kernel, nrow, ncol),
        out_shape=jax.ShapeDtypeStruct(flow_tiles.shape, jnp.float32),
        in_specs=[pl.BlockSpec(memory_space=pl.ANY), pl.BlockSpec(memory_space=pl.ANY)],
        out_specs=pl.BlockSpec(memory_space=pltpu.VMEM),
        scratch_shapes=[
            pltpu.SMEM((1, tiles), jnp.int32),
            pltpu.VMEM((tiles, width, width), jnp.bfloat16),
            pltpu.VMEM((CORES * pieces, depth, width), jnp.bfloat16),
            pltpu.VMEM((nrow, pieces, depth, width), jnp.bfloat16),
            pltpu.VMEM((ncol, tiles, CORES, width, width), jnp.bfloat16),
            pltpu.VMEM((share, CORES, width, width), jnp.float32),
            pltpu.VMEM((share, width, width), jnp.float32),
            pltpu.VMEM((tiles, width, width), jnp.float32),
            pltpu.VMEM((CORES, tiles, width), jnp.float32),
            pltpu.VMEM((nrow, share, width), jnp.float32),
            dma((2,)),
            dma((planes, CORES * pieces)),
            dma((planes, CORES * pieces)),
            dma((pieces,)),
            dma((nrow, pieces)),
            dma((ncol,)),
            dma((CORES, ncol)),
            dma((ncol,)),
            dma((2,)),
            dma((2,)),
            dma((nrow,)),
            dma((nrow,)),
        ],
        compiler_params=pltpu.CompilerParams(
            collective_id=0, has_side_effects=True, vmem_limit_bytes=60 * 1024 * 1024
        ),
        name="cluster_step",
    )(tile_cols, flow_tiles)


def solution(mesh):
    placed = (P("row", "col", None, None), P("row", "col"), P(("row", "col"), None))
    return jax.shard_map(
        functools.partial(on_device, mesh.shape["row"], mesh.shape["col"]),
        mesh=mesh,
        in_specs=placed,
        out_specs=P("row", "col", None, None),
        check_vma=False,
    )
```

```python
import functools
import math

import jax
import jax.numpy as jnp
from jax import lax
from jax.experimental import pallas as pl
from jax.experimental.pallas import tpu as pltpu
from jax.sharding import PartitionSpec as P

MESH = pl.DeviceIdType.MESH
CORES = 2
SPLIT = 2


def remote(src, dst, send_sem, recv_sem, device):
    return pltpu.make_async_remote_copy(
        src_ref=src,
        dst_ref=dst,
        send_sem=send_sem,
        recv_sem=recv_sem,
        device_id=device,
        device_id_type=MESH,
    )


def kernel(
    nrow, ncol, cols_hbm, flow_hbm, squares_ref, scale_ref,
    cols, raw, own, blocks, left, acc, swap, result, placed, flags, sums,
    in_sem, out_sem, up_send, dn_send, mate_send, recv, left_send, left_recv,
    left_mate, flag_sem, swap_sem, sum_send, sum_recv,
):
    tiles, width = raw.shape[0], raw.shape[2]
    depth = own.shape[1]
    share = tiles // CORES
    pieces = share * SPLIT
    planes = nrow // CORES
    row, col = lax.axis_index("row"), lax.axis_index("col")
    z, core = row // CORES, row % CORES
    mate = (row + 1 - 2 * core, col)
    mate_row = row + 1 - 2 * core
    above, below = (row + CORES, col), (row - CORES, col)
    has_above, has_below = z < planes - 1, z > 0
    ny = math.isqrt(ncol)
    ny = ny if ny * ny == ncol else 1
    nx = ncol // ny
    y, x = col // nx, col % nx
    half = tiles // 2

    def at(dy, dx):
        return ((y + dy) % ny) * nx + (x + dx) % nx

    along_x = [(0, dx) for dx in range(1, nx)]
    along_y = [(dy, 0) for dy in range(1, ny)]
    across = [(dy, dx) for dy, _ in along_y for _, dx in along_x]

    load_cols = pltpu.make_async_copy(cols_hbm, cols, in_sem.at[0])
    load_flow = pltpu.make_async_copy(flow_hbm.at[0], raw, in_sem.at[1])
    load_cols.start()
    load_flow.start()

    barrier = pltpu.get_barrier_semaphore()

    def greet(device):
        pl.semaphore_signal(barrier, inc=1, device_id=device, device_id_type=MESH)

    greet(mate)
    for d in along_x + along_y:
        greet((row, at(*d)))

    @pl.when(has_above)
    def _():
        for c in range(CORES):
            greet(((z + 1) * CORES + c, col))

    @pl.when(has_below)
    def _():
        for c in range(CORES):
            greet(((z - 1) * CORES + c, col))

    load_cols.wait()
    load_flow.wait()
    for t in range(tiles):
        target = col + ncol * t
        tile = jnp.zeros((width, width), jnp.float32)
        weight = jnp.float32(0)
        for s in range(tiles):
            w = (cols[0, s] == target).astype(jnp.float32)
            weight = weight + w
            tile = tile + raw[s].astype(jnp.float32) * w
        flags[core, t] = jnp.full((width,), weight, jnp.float32)
        tile = tile.astype(jnp.bfloat16)
        own[t * SPLIT:(t + 1) * SPLIT] = tile.reshape(SPLIT, depth, width)
        left[col, t, core] = tile
    blocks[row] = own[pl.ds(core * pieces, pieces)]

    ends = jnp.where(has_above, 1, 0) + jnp.where(has_below, 1, 0)
    pl.semaphore_wait(barrier, nx + ny - 1 + CORES * ends)

    def piece(src, k, u, send_sem, device):
        return remote(src, blocks.at[k, u], send_sem, recv.at[k, u], device)

    def arrived(k, u):
        piece(own.at[u], k, u, mate_send.at[u], mate).wait_recv()

    def to_mate(u):
        return piece(own.at[(1 - core) * pieces + u], row, u, mate_send.at[u], mate)

    def left_copy(c, t, rc, device, send_sem):
        part = left.at[c, t, rc]
        return remote(part, part, send_sem, left_recv.at[rc, c, t], device)

    def left_out(source, move, t):
        slot = (source[0] + move[0]) * nx + source[1] + move[1]
        return left_copy(at(*source), t, core, (row, at(*move)), left_send.at[slot, t])

    def left_to_mate(source, t):
        c = at(*source)
        return left_copy(c, t, core, mate, left_mate.at[c, t])

    def left_arrived(source, t):
        left_to_mate(source, t).wait_recv()
        left_to_mate(source, t).start()

    def left_relay():
        for t in range(half):
            for d in along_x:
                left_arrived(d, t)
                for move in along_y:
                    left_out(d, move, t).start()
        for t in range(half, tiles):
            for d in along_y:
                left_arrived(d, t)
                for move in along_x:
                    left_out(d, move, t).start()

    flag_copy = remote(flags.at[core], flags.at[core], flag_sem.at[0], flag_sem.at[1], mate)

    for u in range(pieces):
        for c in range(CORES):

            @pl.when(has_above)
            def _():
                piece(
                    own.at[c * pieces + u], row, u, up_send.at[0, c * pieces + u],
                    ((z + 1) * CORES + c, col),
                ).start()

            @pl.when(has_below)
            def _():
                piece(
                    own.at[c * pieces + u], row, u, dn_send.at[0, c * pieces + u],
                    ((z - 1) * CORES + c, col),
                ).start()

        if u == 0:
            for t in range(tiles):
                for d in along_x:
                    left_out((0, 0), d, t).start()
                for d in along_y:
                    left_out((0, 0), d, tiles - 1 - t).start()
    for u in range(pieces):
        to_mate(u).start()
    for t in range(tiles):
        left_to_mate((0, 0), t).start()
    flag_copy.start()

    acc[...] = jnp.zeros_like(acc)

    def relay(step):
        for c in range(CORES):
            if step == 1 and c == CORES - 1:
                left_relay()
            for u in range(pieces):

                @pl.when(z >= step)
                def _():
                    k = (z - step) * CORES + c
                    arrived(k, u)

                    @pl.when(has_above)
                    def _():
                        piece(
                            blocks.at[k, u], k, u, up_send.at[step, c * pieces + u], above
                        ).start()

                @pl.when(z + step < planes)
                def _():
                    k = (z + step) * CORES + c
                    arrived(k, u)

                    @pl.when(has_below)
                    def _():
                        piece(
                            blocks.at[k, u], k, u, dn_send.at[step, c * pieces + u], below
                        ).start()

    def multiply(k):
        a = left[k % ncol, k // ncol].reshape(CORES * width, width)
        for i in range(share):
            b = blocks[k, pl.ds(i * SPLIT, SPLIT)].reshape(width, width)
            c = jnp.dot(a, b, preferred_element_type=jnp.float32)
            acc[i] += c.reshape(CORES, width, width)

    def multiply_piece(k, u):
        h = u % SPLIT
        a = left[k % ncol, k // ncol, :, :, pl.ds(h * depth, depth)]
        c = jnp.dot(
            a.reshape(CORES * width, depth), blocks[k, u], preferred_element_type=jnp.float32
        )
        acc[u // SPLIT] += c.reshape(CORES, width, width)

    def compute(distance):
        for sign in (-1, 1) if distance else (1,):
            plane = z + sign * distance

            @pl.when((plane >= 0) & (plane < planes))
            def _():
                if distance == 0:
                    for u in range(pieces):
                        arrived(mate_row, u)
                for c in range(CORES):
                    multiply(plane * CORES + c)

    def last(distance):
        for sign in (-1, 1):
            plane = z + sign * distance

            @pl.when((plane >= 0) & (plane < planes))
            def _():
                for c in range(CORES):
                    for u in range(pieces):
                        k = plane * CORES + c
                        arrived(k, u)
                        multiply_piece(k, u)

    done = 0

    def catch_up(upto):
        nonlocal done
        if done == 0:
            for d in across:
                for t in range(tiles):
                    left_arrived(d, t)
            for c in range(ncol):
                for t in range(tiles):
                    left_copy(c, t, 1 - core, mate, left_mate.at[c, t]).wait_recv()
        while done < upto:
            compute(done)
            done += 1

    for step in range(1, planes - 1):
        if step > 2:
            catch_up(step)
        relay(step)
        if step == 1:
            for t in range(half, tiles):
                for d in along_x:
                    left_arrived(d, t)
            for t in range(half):
                for d in along_y:
                    left_arrived(d, t)
    catch_up(planes - 1)
    last(planes - 1)
    flag_copy.wait_recv()

    for i in range(share):
        t = core * share + i
        part = jnp.zeros((width,), jnp.float32)
        for c in range(CORES):
            part = part + jnp.sum(acc[i, c] * acc[i, c], axis=0) * flags[c, t]
        sums[row, i] = part

    def to_row(d):
        return remote(
            sums.at[row], sums.at[row], sum_send.at[d], sum_recv.at[row],
            ((row + d) % nrow, col),
        )

    for d in range(1, nrow):
        to_row(d).start()

    for i in range(share):
        other = acc[i, 1 - core]
        swap[i] = other * other
    swap_copy = remote(
        swap, result.at[pl.ds(core * share, share)], swap_sem.at[0], swap_sem.at[1], mate
    )
    swap_copy.start()
    for i in range(share):
        mine = acc[i, core]
        result[core * share + i] = mine * mine
    swap_copy.wait_recv()

    weights = [
        [(cols[0, s] == col + ncol * t).astype(jnp.float32) for t in range(tiles)]
        for s in range(tiles)
    ]
    for s in range(tiles):
        chosen = jnp.zeros((width, width), jnp.float32)
        for t in range(tiles):
            chosen = chosen + result[t] * weights[s][t]
        placed[s] = chosen
    store = pltpu.make_async_copy(placed, squares_ref.at[0], out_sem)
    store.start()

    for d in range(1, nrow):
        other = (row + d) % nrow
        remote(
            sums.at[other], sums.at[other], sum_send.at[d], sum_recv.at[other], (other, col)
        ).wait_recv()
    scales = []
    for t in range(tiles):
        total = sums[t // share, t % share]
        for p in range(1, planes):
            total = total + sums[p * CORES + t // share, t % share]
        safe = jnp.where(total > 0, total, 1.0)
        scales.append(jnp.float32(0.5 * nrow * width) / safe)
    for s in range(tiles):
        scale = jnp.zeros((width,), jnp.float32)
        for t in range(tiles):
            scale = scale + scales[t] * weights[s][t]
        scale_ref[s] = scale
        scale_ref[tiles + s] = jnp.full((width,), 0.5 * sum(weights[s]), jnp.float32)
    store.wait()
    for n in range(CORES * pieces):
        for step in range(planes):

            @pl.when(has_above & (z >= step))
            def _():
                piece(own.at[n], row, 0, up_send.at[step, n], above).wait_send()

            @pl.when(has_below & (z + step < planes))
            def _():
                piece(own.at[n], row, 0, dn_send.at[step, n], below).wait_send()

    for u in range(pieces):
        to_mate(u).wait_send()
    for t in range(tiles):
        for d in along_x + along_y:
            left_out((0, 0), d, t).wait_send()
        for dy, dx in across:
            source, move = ((0, dx), (dy, 0)) if t < half else ((dy, 0), (0, dx))
            left_out(source, move, t).wait_send()
        for c in range(ncol):
            left_copy(c, t, core, mate, left_mate.at[c, t]).wait_send()
    flag_copy.wait_send()
    swap_copy.wait_send()
    for d in range(1, nrow):
        to_row(d).wait_send()


def on_device(nrow, ncol, flow_tiles, tile_cols, pairs):
    _, tiles, _, width = flow_tiles.shape
    planes, depth, share = nrow // CORES, width // SPLIT, tiles // CORES
    pieces = share * SPLIT
    dma = pltpu.SemaphoreType.DMA
    squares, scale = pl.pallas_call(
        functools.partial(kernel, nrow, ncol),
        out_shape=(
            jax.ShapeDtypeStruct(flow_tiles.shape, jnp.float32),
            jax.ShapeDtypeStruct((2 * tiles, width), jnp.float32),
        ),
        in_specs=[pl.BlockSpec(memory_space=pltpu.HBM)] * 2,
        out_specs=(
            pl.BlockSpec(memory_space=pltpu.HBM), pl.BlockSpec(memory_space=pltpu.VMEM)
        ),
        scratch_shapes=[
            pltpu.SMEM((1, tiles), jnp.int32),
            pltpu.VMEM((tiles, width, width), jnp.bfloat16),
            pltpu.VMEM((CORES * pieces, depth, width), jnp.bfloat16),
            pltpu.VMEM((nrow, pieces, depth, width), jnp.bfloat16),
            pltpu.VMEM((ncol, tiles, CORES, width, width), jnp.bfloat16),
            pltpu.VMEM((share, CORES, width, width), jnp.float32),
            pltpu.VMEM((share, width, width), jnp.float32),
            pltpu.VMEM((tiles, width, width), jnp.float32),
            pltpu.VMEM((tiles, width, width), jnp.float32),
            pltpu.VMEM((CORES, tiles, width), jnp.float32),
            pltpu.VMEM((nrow, share, width), jnp.float32),
            dma((2,)),
            dma,
            dma((planes, CORES * pieces)),
            dma((planes, CORES * pieces)),
            dma((pieces,)),
            dma((nrow, pieces)),
            dma((ncol, tiles)),
            dma((CORES, ncol, tiles)),
            dma((ncol, tiles)),
            dma((2,)),
            dma((2,)),
            dma((nrow,)),
            dma((nrow,)),
        ],
        compiler_params=pltpu.CompilerParams(
            collective_id=0, has_side_effects=True, vmem_limit_bytes=60 * 1024 * 1024
        ),
        name="cluster_step",
    )(tile_cols, flow_tiles)
    return (
        flow_tiles.astype(jnp.float32) * scale[None, tiles:, None, :]
        + squares * scale[None, :tiles, None, :]
    )


def solution(mesh):
    placed = (P("row", "col", None, None), P("row", "col"), P(("row", "col"), None))
    return jax.shard_map(
        functools.partial(on_device, mesh.shape["row"], mesh.shape["col"]),
        mesh=mesh,
        in_specs=placed,
        out_specs=P("row", "col", None, None),
        check_vma=False,
    )
```

```python
import functools
import math

import jax
import jax.numpy as jnp
from jax import lax
from jax.experimental import pallas as pl
from jax.experimental.pallas import tpu as pltpu
from jax.sharding import PartitionSpec as P

MESH = pl.DeviceIdType.MESH
CORES = 2
SPLIT = 2


def remote(src, dst, send_sem, recv_sem, device):
    return pltpu.make_async_remote_copy(
        src_ref=src,
        dst_ref=dst,
        send_sem=send_sem,
        recv_sem=recv_sem,
        device_id=device,
        device_id_type=MESH,
    )


def kernel(
    nrow, ncol, cols_hbm, flow_hbm, out_ref,
    cols, raw, own, blocks, left, acc, swap, result, flags, sums,
    in_sem, up_send, dn_send, mate_send, recv, left_send, left_recv,
    left_mate, flag_sem, swap_sem, sum_send, sum_recv,
):
    tiles, width = raw.shape[0], raw.shape[2]
    depth = own.shape[1]
    share = tiles // CORES
    pieces = share * SPLIT
    planes = nrow // CORES
    row, col = lax.axis_index("row"), lax.axis_index("col")
    z, core = row // CORES, row % CORES
    mate = (row + 1 - 2 * core, col)
    mate_row = row + 1 - 2 * core
    above, below = (row + CORES, col), (row - CORES, col)
    has_above, has_below = z < planes - 1, z > 0
    ny = math.isqrt(ncol)
    ny = ny if ny * ny == ncol else 1
    nx = ncol // ny
    y, x = col // nx, col % nx
    half = tiles // 2

    def at(dy, dx):
        return ((y + dy) % ny) * nx + (x + dx) % nx

    along_x = [(0, dx) for dx in range(1, nx)]
    along_y = [(dy, 0) for dy in range(1, ny)]
    across = [(dy, dx) for dy, _ in along_y for _, dx in along_x]

    load_cols = pltpu.make_async_copy(cols_hbm, cols, in_sem.at[0])
    load_flow = pltpu.make_async_copy(flow_hbm.at[0], raw, in_sem.at[1])
    load_cols.start()
    load_flow.start()

    barrier = pltpu.get_barrier_semaphore()

    def greet(device):
        pl.semaphore_signal(barrier, inc=1, device_id=device, device_id_type=MESH)

    greet(mate)
    for d in along_x + along_y:
        greet((row, at(*d)))

    @pl.when(has_above)
    def _():
        for c in range(CORES):
            greet(((z + 1) * CORES + c, col))

    @pl.when(has_below)
    def _():
        for c in range(CORES):
            greet(((z - 1) * CORES + c, col))

    load_cols.wait()
    load_flow.wait()
    for t in range(tiles):
        target = col + ncol * t
        tile = jnp.zeros((width, width), jnp.float32)
        weight = jnp.float32(0)
        for s in range(tiles):
            w = (cols[0, s] == target).astype(jnp.float32)
            weight = weight + w
            tile = tile + raw[s].astype(jnp.float32) * w
        flags[core, t] = jnp.full((width,), weight, jnp.float32)
        tile = tile.astype(jnp.bfloat16)
        own[t * SPLIT:(t + 1) * SPLIT] = tile.reshape(SPLIT, depth, width)
        left[col, t, core] = tile
    blocks[row] = own[pl.ds(core * pieces, pieces)]

    ends = jnp.where(has_above, 1, 0) + jnp.where(has_below, 1, 0)
    pl.semaphore_wait(barrier, nx + ny - 1 + CORES * ends)

    def piece(src, k, u, send_sem, device):
        return remote(src, blocks.at[k, u], send_sem, recv.at[k, u], device)

    def arrived(k, u):
        piece(own.at[u], k, u, mate_send.at[u], mate).wait_recv()

    def to_mate(u):
        return piece(own.at[(1 - core) * pieces + u], row, u, mate_send.at[u], mate)

    def left_copy(c, t, rc, device, send_sem):
        part = left.at[c, t, rc]
        return remote(part, part, send_sem, left_recv.at[rc, c, t], device)

    def left_out(source, move, t):
        slot = (source[0] + move[0]) * nx + source[1] + move[1]
        return left_copy(at(*source), t, core, (row, at(*move)), left_send.at[slot, t])

    def left_to_mate(source, t):
        c = at(*source)
        return left_copy(c, t, core, mate, left_mate.at[c, t])

    def left_arrived(source, t):
        left_to_mate(source, t).wait_recv()
        left_to_mate(source, t).start()

    def left_relay():
        for t in range(half):
            for d in along_x:
                left_arrived(d, t)
                for move in along_y:
                    left_out(d, move, t).start()
        for t in range(half, tiles):
            for d in along_y:
                left_arrived(d, t)
                for move in along_x:
                    left_out(d, move, t).start()

    flag_copy = remote(flags.at[core], flags.at[core], flag_sem.at[0], flag_sem.at[1], mate)

    for u in range(pieces):
        for c in range(CORES):

            @pl.when(has_above)
            def _():
                piece(
                    own.at[c * pieces + u], row, u, up_send.at[0, c * pieces + u],
                    ((z + 1) * CORES + c, col),
                ).start()

            @pl.when(has_below)
            def _():
                piece(
                    own.at[c * pieces + u], row, u, dn_send.at[0, c * pieces + u],
                    ((z - 1) * CORES + c, col),
                ).start()

        if u == 0:
            for t in range(tiles):
                for d in along_x:
                    left_out((0, 0), d, t).start()
                for d in along_y:
                    left_out((0, 0), d, tiles - 1 - t).start()
    for u in range(pieces):
        to_mate(u).start()
    for t in range(tiles):
        left_to_mate((0, 0), t).start()
    flag_copy.start()

    acc[...] = jnp.zeros_like(acc)

    def relay(step):
        for c in range(CORES):
            if step == 1 and c == CORES - 1:
                left_relay()
            for u in range(pieces):

                @pl.when(z >= step)
                def _():
                    k = (z - step) * CORES + c
                    arrived(k, u)

                    @pl.when(has_above)
                    def _():
                        piece(
                            blocks.at[k, u], k, u, up_send.at[step, c * pieces + u], above
                        ).start()

                @pl.when(z + step < planes)
                def _():
                    k = (z + step) * CORES + c
                    arrived(k, u)

                    @pl.when(has_below)
                    def _():
                        piece(
                            blocks.at[k, u], k, u, dn_send.at[step, c * pieces + u], below
                        ).start()

    def multiply(k):
        a = left[k % ncol, k // ncol].reshape(CORES * width, width)
        for i in range(share):
            b = blocks[k, pl.ds(i * SPLIT, SPLIT)].reshape(width, width)
            c = jnp.dot(a, b, preferred_element_type=jnp.float32)
            acc[i] += c.reshape(CORES, width, width)

    def multiply_piece(k, u):
        h = u % SPLIT
        a = left[k % ncol, k // ncol, :, :, pl.ds(h * depth, depth)]
        c = jnp.dot(
            a.reshape(CORES * width, depth), blocks[k, u], preferred_element_type=jnp.float32
        )
        acc[u // SPLIT] += c.reshape(CORES, width, width)

    def compute(distance):
        for sign in (-1, 1) if distance else (1,):
            plane = z + sign * distance

            @pl.when((plane >= 0) & (plane < planes))
            def _():
                if distance == 0:
                    for u in range(pieces):
                        arrived(mate_row, u)
                for c in range(CORES):
                    multiply(plane * CORES + c)

    def last(distance):
        for sign in (-1, 1):
            plane = z + sign * distance

            @pl.when((plane >= 0) & (plane < planes))
            def _():
                for c in range(CORES):
                    for u in range(pieces):
                        k = plane * CORES + c
                        arrived(k, u)
                        multiply_piece(k, u)

    done = 0

    def catch_up(upto):
        nonlocal done
        if done == 0:
            for d in across:
                for t in range(tiles):
                    left_arrived(d, t)
            for c in range(ncol):
                for t in range(tiles):
                    left_copy(c, t, 1 - core, mate, left_mate.at[c, t]).wait_recv()
        while done < upto:
            compute(done)
            done += 1

    for step in range(1, planes - 1):
        if step > 2:
            catch_up(step)
        relay(step)
        if step == 1:
            for t in range(half, tiles):
                for d in along_x:
                    left_arrived(d, t)
            for t in range(half):
                for d in along_y:
                    left_arrived(d, t)
    catch_up(planes - 1)
    last(planes - 1)
    flag_copy.wait_recv()

    for i in range(share):
        t = core * share + i
        part = jnp.zeros((width,), jnp.float32)
        for c in range(CORES):
            part = part + jnp.sum(acc[i, c] * acc[i, c], axis=0) * flags[c, t]
        sums[row, i] = part

    def to_row(d):
        return remote(
            sums.at[row], sums.at[row], sum_send.at[d], sum_recv.at[row],
            ((row + d) % nrow, col),
        )

    for d in range(1, nrow):
        to_row(d).start()

    for i in range(share):
        other = acc[i, 1 - core]
        swap[i] = other * other
    swap_copy = remote(
        swap, result.at[pl.ds(core * share, share)], swap_sem.at[0], swap_sem.at[1], mate
    )
    swap_copy.start()
    for i in range(share):
        mine = acc[i, core]
        result[core * share + i] = mine * mine
    swap_copy.wait_recv()

    for d in range(1, nrow):
        other = (row + d) % nrow
        remote(
            sums.at[other], sums.at[other], sum_send.at[d], sum_recv.at[other], (other, col)
        ).wait_recv()
    for s in range(tiles):
        out = jnp.zeros((width, width), jnp.float32)
        held = jnp.float32(0)
        for t in range(tiles):
            w = (cols[0, s] == col + ncol * t).astype(jnp.float32)
            held = held + w
            total = sums[t // share, t % share]
            for p in range(1, planes):
                total = total + sums[p * CORES + t // share, t % share]
            safe = jnp.where(total > 0, total, 1.0)
            scale = jnp.float32(0.5 * nrow * width) / safe * w
            out = out + result[t] * scale[None, :]
        out_ref[0, s] = out + raw[s].astype(jnp.float32) * (0.5 * held)
    for n in range(CORES * pieces):
        for step in range(planes):

            @pl.when(has_above & (z >= step))
            def _():
                piece(own.at[n], row, 0, up_send.at[step, n], above).wait_send()

            @pl.when(has_below & (z + step < planes))
            def _():
                piece(own.at[n], row, 0, dn_send.at[step, n], below).wait_send()

    for u in range(pieces):
        to_mate(u).wait_send()
    for t in range(tiles):
        for d in along_x + along_y:
            left_out((0, 0), d, t).wait_send()
        for dy, dx in across:
            source, move = ((0, dx), (dy, 0)) if t < half else ((dy, 0), (0, dx))
            left_out(source, move, t).wait_send()
        for c in range(ncol):
            left_copy(c, t, core, mate, left_mate.at[c, t]).wait_send()
    flag_copy.wait_send()
    swap_copy.wait_send()
    for d in range(1, nrow):
        to_row(d).wait_send()


def on_device(nrow, ncol, flow_tiles, tile_cols, pairs):
    _, tiles, _, width = flow_tiles.shape
    planes, depth, share = nrow // CORES, width // SPLIT, tiles // CORES
    pieces = share * SPLIT
    dma = pltpu.SemaphoreType.DMA
    return pl.pallas_call(
        functools.partial(kernel, nrow, ncol),
        out_shape=jax.ShapeDtypeStruct(flow_tiles.shape, jnp.float32),
        in_specs=[pl.BlockSpec(memory_space=pltpu.HBM)] * 2,
        out_specs=pl.BlockSpec(memory_space=pltpu.VMEM),
        scratch_shapes=[
            pltpu.SMEM((1, tiles), jnp.int32),
            pltpu.VMEM((tiles, width, width), jnp.bfloat16),
            pltpu.VMEM((CORES * pieces, depth, width), jnp.bfloat16),
            pltpu.VMEM((nrow, pieces, depth, width), jnp.bfloat16),
            pltpu.VMEM((ncol, tiles, CORES, width, width), jnp.bfloat16),
            pltpu.VMEM((share, CORES, width, width), jnp.float32),
            pltpu.VMEM((share, width, width), jnp.float32),
            pltpu.VMEM((tiles, width, width), jnp.float32),
            pltpu.VMEM((CORES, tiles, width), jnp.float32),
            pltpu.VMEM((nrow, share, width), jnp.float32),
            dma((2,)),
            dma((planes, CORES * pieces)),
            dma((planes, CORES * pieces)),
            dma((pieces,)),
            dma((nrow, pieces)),
            dma((ncol, tiles)),
            dma((CORES, ncol, tiles)),
            dma((ncol, tiles)),
            dma((2,)),
            dma((2,)),
            dma((nrow,)),
            dma((nrow,)),
        ],
        compiler_params=pltpu.CompilerParams(
            collective_id=0, has_side_effects=True, vmem_limit_bytes=24 * 1024 * 1024
        ),
        name="cluster_step",
    )(tile_cols, flow_tiles)


def solution(mesh):
    placed = (P("row", "col", None, None), P("row", "col"), P(("row", "col"), None))
    return jax.shard_map(
        functools.partial(on_device, mesh.shape["row"], mesh.shape["col"]),
        mesh=mesh,
        in_specs=placed,
        out_specs=P("row", "col", None, None),
        check_vma=False,
    )
```
